32 devices in a mesh: ka: 8 (over y, x, core), ga: 4 (over z).
Axes of the slice: x: 2, y: 2, z: 4, core: 2. Of those that a mesh axis runs over, the one named last changes fastest.
Arguments:
- pair_densities: float32 [8192, 8192], P('ka', 'ga'), may hold values from -0.0625 to 0.0625
- energies: float32 [8192], P('ka'), may hold values from -2 to 2
- coulomb: float32 [8192], P('ga'), may hold values from 0.2 to 2
- start: float32 [8192, 128], P('ka'), may hold values from -6 to 6
Outputs:
- alphas: float32 [4, 128], replicated
- betas: float32 [4, 128], replicated
- lanczos_vector: float32 [8192, 128], P('ka')
The draws below stay inside these ranges and needn't reach their ends.
All inputs are finite; a program needn't handle non-finite values.
Results may differ from the reference program's by a relative error of at most 0.00013.
Values sent between devices are 32-bit elements; how exact they have to be, the bound alone decides.
A program may use at most 64 MiB of HBM per device.

```python
import math
import jax
import jax.numpy as jnp
from jax import lax

G = 8192
NV = 128
ITERS = 4
ROWS = 8192


def levels(stream_key, dims, pieces, smallest, high):
    factor_of = 1.0
    for dim, blocks in pieces:
        heights = jax.random.uniform(jax.random.fold_in(jax.random.fold_in(stream_key, 6), dim), (blocks,), jnp.float32, smallest / len(pieces), high / len(pieces))
        factor_of = factor_of * jnp.repeat(jnp.exp(heights), dims[dim] // blocks).reshape((-1,) + (1,) * (len(dims) - 1 - dim))
    return factor_of


def scatter_about(rng, dims, deviation, most, split=(), dtype=jnp.bfloat16):
    entries = deviation * jax.random.normal(rng, dims, jnp.float32)
    if split:
        entries = entries * levels(rng, dims, split, -0.22, 0.18)
    return jnp.clip(entries, -most, most).astype(dtype)


def setup_inputs(seed: int = 0) -> dict:
    key_list = jax.random.split(jax.random.key(seed), 5)
    pair_densities = scatter_about(key_list[0], (ROWS, G), ROWS ** -0.5, 0.0625, ((0, 8), (1, 4)), jnp.float32)
    energies = jnp.clip(jax.random.uniform(key_list[1], (ROWS,), jnp.float32, -2.0, 2.0) * levels(key_list[1], (ROWS,), ((0, 8),), -0.4, 0.0), -2.0, 2.0)
    coulomb = jnp.clip(jnp.exp(math.log(2.0) - 2.3025851 * jax.random.uniform(key_list[2], (G,), jnp.float32) ** levels(key_list[2], (G,), ((0, 4),), -0.2, 0.2)), 0.2, 2.0)
    start = scatter_about(key_list[3], (ROWS, NV), 1.0, 6.0, ((0, 8),), jnp.float32)
    return {"pair_densities": pair_densities, "energies": energies, "coulomb": coulomb, "start": start}


EPSILON = 1e-06

def reference(pair_densities, energies, coulomb, start):
    precise = lax.Precision.HIGHEST

    def apply_ham(vector):
        projected = jnp.dot(pair_densities.T, vector, precision=precise, preferred_element_type=jnp.float32)
        weighted = coulomb[:, None] * projected
        mixed = jnp.dot(pair_densities, weighted, precision=precise, preferred_element_type=jnp.float32)
        return energies[:, None] * vector + mixed
    vector = start / jnp.sqrt(lax.optimization_barrier(jnp.sum(start * start, axis=0)) + EPSILON)
    previous = jnp.zeros_like(vector)
    beta_now = jnp.zeros((vector.shape[1],), jnp.float32)
    alpha_rows = []
    beta_rows = []
    for step in range(ITERS):
        image = apply_ham(vector)
        alpha_now = lax.optimization_barrier(jnp.sum(vector * image, axis=0))
        remainder = image - alpha_now * vector - beta_now * previous
        beta_new = jnp.sqrt(lax.optimization_barrier(jnp.sum(remainder * remainder, axis=0)) + EPSILON)
        previous = vector
        vector = remainder / beta_new
        beta_now = beta_new
        alpha_rows.append(alpha_now)
        beta_rows.append(beta_new)
    return (jnp.stack(alpha_rows), jnp.stack(beta_rows), vector)
```

```python
import functools

import jax
import jax.numpy as jnp
from jax import lax
from jax.experimental import pallas as pl
from jax.experimental.pallas import tpu as pltpu
from jax.sharding import PartitionSpec as P

ITERS = 4
EPSILON = 1e-06
MESH = pl.DeviceIdType.MESH
F32 = jnp.float32
BF16 = jnp.bfloat16
NT = (((1,), (1,)), ((), ()))
NN = (((1,), (0,)), ((), ()))


def split(x):
    hi = x.astype(BF16)
    return hi, (x - hi.astype(F32)).astype(BF16)


def dot3(x_hi_lo, x_hi, w_hi, w_lo, dims):
    n = x_hi.shape[0]
    both = lax.dot_general(x_hi_lo, w_hi, dims, preferred_element_type=F32)
    low = lax.dot_general(x_hi, w_lo, dims, preferred_element_type=F32)
    return both[:n] + both[n:] + low


def kernel(nka, nga, cfg, m_ref, e_ref, c_ref, s_ref, al_ref, be_ref, out_ref,
           mhi, mlo, r, prev, xs, ws, tx, rx, acc, full, ypart, rtx, ltx, rrx, lrx,
           row_tx, ka_rx, ga_tx, ga_rx, *rest):
    nb, gw, cw, nch, nv = cfg
    stage_rx = rest[:nb]
    (core_ss, core_rs, st_ss, st_rs, ag_ss, ag_rs, fin_ss, fin_rs,
     r_ss, r_rs, l_ss, l_rs, ka_ss, ka_rs, ga_ss, ga_rs) = rest[nb:]
    ka = lax.axis_index("ka")
    ga = lax.axis_index("ga")
    core = ka % 2
    rows, gs = m_ref.shape
    gh = gs // 2

    def flip(mask):
        return ka + mask - 2 * mask * ((ka // mask) % 2)

    def bit_of(mask):
        return (ka // mask) % 2

    partners, bits = [], []
    for t in range(nb):
        a, b = 2 << t, 2 << (nb - 1 - t)
        partners.append(flip(a) + core * (flip(b) - flip(a)))
        bits.append(bit_of(a) + core * (bit_of(b) - bit_of(a)))

    barrier = pltpu.get_barrier_semaphore()
    for i in range(1, nka):
        pl.semaphore_signal(barrier, inc=1, device_id=((ka + i) % nka, ga), device_id_type=MESH)
    for i in range(1, nga):
        pl.semaphore_signal(barrier, inc=1, device_id=(ka, (ga + i) % nga), device_id_type=MESH)

    @pl.loop(0, rows // 128)
    def _(i):
        sl = pl.ds(pl.multiple_of(i * 128, 128), 128)
        hi, lo = split(m_ref[sl, :])
        mhi[sl, :] = hi
        mlo[sl, :] = lo
        r[:, sl] = s_ref[sl, :].T

    prev[...] = jnp.zeros_like(prev)
    pl.semaphore_wait(barrier, nka - 1 + nga - 1)

    def copy(src, dst, ss, rs, dev):
        return pltpu.make_async_remote_copy(
            src_ref=src, dst_ref=dst, send_sem=ss, recv_sem=rs, device_id=dev, device_id_type=MESH)

    def fold(x):
        parts = x[:, :128]
        for i in range(1, x.shape[1] // 128):
            parts = parts + x[:, i * 128:(i + 1) * 128]
        return jnp.sum(parts.T, axis=0, keepdims=True)

    def column(row):
        return jnp.broadcast_to(row, (128, nv)).T

    def wide(col, width):
        return jnp.concatenate([col] * (width // 128), axis=1)

    def small_copies(src, dst, ss, rs, n, me, dev, par):
        return [copy(src.at[par], dst.at[par, i], ss.at[i], rs.at[par, i], dev((me + i) % n))
                for i in range(1, n)]

    def ka_small(par):
        return small_copies(row_tx, ka_rx, ka_ss, ka_rs, nka, ka, lambda d: (d, ga), par)

    def ga_small(par):
        return small_copies(ga_tx, ga_rx, ga_ss, ga_rs, nga, ga, lambda d: (ka, d), par)

    def finish(copies, src, dst, n, par):
        for c in copies:
            c.wait()
        total = src[par]
        for i in range(1, n):
            total = total + dst[par, i]
        return total

    def project(half, write):
        @pl.loop(0, gh // gw)
        def _(i):
            dst = pl.ds(pl.multiple_of(i * gw, gw), gw)
            sl = pl.ds(pl.multiple_of(half * gh + i * gw, gw), gw)
            write(dst, dot3(xs[...], xs[:nv, :], mhi[:, sl], mlo[:, sl], NN))

    def body(k, carry):
        par = k % 2
        x = r[...]
        hi, lo = split(x)
        xs[:nv, :] = hi
        xs[nv:, :] = lo
        sq = x * x
        row_tx[par, 0:1, :] = fold(sq)
        row_tx[par, 1:2, :] = fold(e_ref[...] * sq)
        sums = ka_small(par)
        for c in sums:
            c.start()

        def to_tx(dst, y):
            tx[:, dst] = y

        def to_acc(dst, y):
            acc[:, dst] = y

        other = ka + 1 - 2 * core
        project(1 - core, to_tx)
        first = copy(tx, rx.at[par], core_ss.at[0], core_rs.at[par], (other, ga))
        first.start()
        project(core, to_acc)
        first.wait()
        acc[...] += rx[par]

        off, size = 0, nv
        spans = []
        for t in range(nb - 1):
            size //= 2
            keep = pl.multiple_of(off + bits[t] * size, 8)
            give = pl.multiple_of(off + (1 - bits[t]) * size, 8)
            c = copy(acc.at[pl.ds(give, size), :], stage_rx[t].at[par], st_ss.at[t], st_rs.at[par, t],
                     (partners[t], ga))
            c.start()
            c.wait()
            acc[pl.ds(keep, size), :] += stage_rx[t][par]
            off = keep
            spans.append((keep, size))
        t = nb - 1
        mine = pl.ds(off, size)
        c = copy(acc.at[mine, :], stage_rx[t].at[par], st_ss.at[t], st_rs.at[par, t], (partners[t], ga))
        c.start()
        c.wait()
        full[par, core, mine, :] = acc[mine, :] + stage_rx[t][par]
        for t in reversed(range(nb - 1)):
            keep, size = spans[t]
            part = full.at[par, core, pl.ds(keep, size), :]
            c = copy(part, part, ag_ss.at[t], ag_rs.at[par, t], (partners[t], ga))
            c.start()
            c.wait()
        part = full.at[par, core]
        c = copy(part, part, fin_ss.at[0], fin_rs.at[par], (other, ga))
        c.start()

        total = finish(sums, row_tx, ka_rx, nka, par)
        beta = jnp.sqrt(total[0:1] + EPSILON)
        energy = total[1:2] / (beta * beta)
        be_ref[pl.ds(jnp.maximum(k - 1, 0), 1), :] = beta
        beta_col = column(beta)
        c.wait()

        curve = jnp.zeros((nv, 128), F32)
        for h in range(2):
            for i in range(gh // 128):
                sl = slice(i * 128, (i + 1) * 128)
                gsl = slice(h * gh + i * 128, h * gh + (i + 1) * 128)
                p = full[par, h, :, sl] / beta_col
                w = c_ref[:, gsl] * p
                curve = curve + p * w
                hi, lo = split(w)
                ws[:nv, gsl] = hi
                ws[nv:, gsl] = lo
        ga_tx[par, 0:1, :] = fold(curve)
        curves = ga_small(par)
        for c in curves:
            c.start()

        def right(j):
            return copy(rtx.at[j], rrx.at[par, j], r_ss.at[j], r_rs.at[par, j], (ka, ga + 1))

        def left(j):
            return copy(ltx.at[j], lrx.at[par, j], l_ss.at[j], l_rs.at[par, j], (ka, ga - 1))

        @pl.loop(0, nch)
        def _(j):
            sl = pl.ds(pl.multiple_of(j * cw, cw), cw)
            y = dot3(ws[...], ws[:nv, :], mhi[sl, :], mlo[sl, :], NT)
            ypart[j] = y

            @pl.when(ga == 0)
            def _():
                rtx[j] = y
                right(j).start()

            @pl.when(ga == nga - 1)
            def _():
                ltx[j] = y
                left(j).start()

        beta_wide = wide(beta_col, rows)
        r[...] = r[...] / beta_wide
        for j in range(nch):
            @pl.when(ga > 0)
            def _():
                right(j).wait_recv()

                @pl.when(ga < nga - 1)
                def _():
                    rtx[j] = rrx[par, j] + ypart[j]
                    right(j).start()

            @pl.when(ga < nga - 1)
            def _():
                left(j).wait_recv()

                @pl.when(ga > 0)
                def _():
                    ltx[j] = lrx[par, j] + ypart[j]
                    left(j).start()

        alpha = energy + finish(curves, ga_tx, ga_rx, nga, par)[0:1]
        al_ref[pl.ds(k, 1), :] = alpha
        alpha_col = wide(column(alpha), cw)
        beta_col = wide(beta_col, cw)
        for j in range(nch):
            sl = slice(j * cw, (j + 1) * cw)

            @pl.when(ga > 0)
            def _():
                ypart[j] += rrx[par, j]

            @pl.when(ga < nga - 1)
            def _():
                ypart[j] += lrx[par, j]

            v = r[:, sl]
            new = (e_ref[:, sl] - alpha_col) * v + ypart[j] - beta_col * prev[:, sl]
            prev[:, sl] = v
            r[:, sl] = new
        for j in range(nch):
            @pl.when(ga < nga - 1)
            def _():
                right(j).wait_send()

            @pl.when(ga > 0)
            def _():
                left(j).wait_send()
        return carry

    lax.fori_loop(0, ITERS, body, 0)
    par = ITERS % 2
    x = r[...]
    row_tx[par, 0:1, :] = fold(x * x)
    sums = ka_small(par)
    for c in sums:
        c.start()
    total = finish(sums, row_tx, ka_rx, nka, par)
    beta = jnp.sqrt(total[0:1] + EPSILON)
    be_ref[ITERS - 1:ITERS, :] = beta
    for j in range(rows // 128):
        sl = slice(j * 128, (j + 1) * 128)
        out_ref[sl, :] = r[:, sl].T / beta


def solution(mesh):
    nka, nga = mesh.shape["ka"], mesh.shape["ga"]
    nb = (nka // 2).bit_length() - 1

    def step(m, e, c, s):
        rows, gs = m.shape
        nv = s.shape[1]
        gh = gs // 2
        gw = min(512, gh)
        cw = 256
        nch = rows // cw
        stage = []
        for t in range(nb):
            size = nv >> (t + 1) if t < nb - 1 else nv >> (nb - 1)
            stage.append(pltpu.VMEM((2, size, gh), F32))
        vm = pltpu.VMEM
        dma = pltpu.SemaphoreType.DMA
        return pl.pallas_call(
            functools.partial(kernel, nka, nga, (nb, gw, cw, nch, nv)),
            out_shape=(jax.ShapeDtypeStruct((ITERS, nv), F32), jax.ShapeDtypeStruct((ITERS, nv), F32),
                       jax.ShapeDtypeStruct((rows, nv), F32)),
            in_specs=[pl.BlockSpec(memory_space=pltpu.VMEM)] * 4,
            out_specs=(pl.BlockSpec(memory_space=pltpu.VMEM),) * 3,
            scratch_shapes=[
                vm((rows, gs), BF16), vm((rows, gs), BF16), vm((nv, rows), F32), vm((nv, rows), F32),
                vm((2 * nv, rows), BF16), vm((2 * nv, gs), BF16),
                vm((nv, gh), F32), vm((2, nv, gh), F32), vm((nv, gh), F32), vm((2, 2, nv, gh), F32),
                vm((nch, nv, cw), F32), vm((nch, nv, cw), F32), vm((nch, nv, cw), F32),
                vm((2, nch, nv, cw), F32), vm((2, nch, nv, cw), F32),
                vm((2, 8, nv), F32), vm((2, nka, 8, nv), F32), vm((2, 8, nv), F32), vm((2, nga, 8, nv), F32),
            ] + stage + [
                dma((1,)), dma((2,)), dma((nb,)), dma((2, nb)), dma((nb,)), dma((2, nb)), dma((1,)), dma((2,)),
                dma((nch,)), dma((2, nch)), dma((nch,)), dma((2, nch)),
                dma((nka,)), dma((2, nka)), dma((nga,)), dma((2, nga)),
            ],
            compiler_params=pltpu.CompilerParams(
                collective_id=0, has_side_effects=True, vmem_limit_bytes=60 * 1024 * 1024),
        )(m, e[None, :], c[None, :], s)

    placed = (P("ka", "ga"), P("ka"), P("ga"), P("ka", None))
    return jax.shard_map(
        step, mesh=mesh, in_specs=placed, out_specs=(P(), P(), P("ka", None)), check_vma=False)
```

```python
import functools

import jax
import jax.numpy as jnp
from jax import lax
from jax.experimental import pallas as pl
from jax.experimental.pallas import tpu as pltpu
from jax.sharding import PartitionSpec as P

ITERS = 4
EPSILON = 1e-06
MESH = pl.DeviceIdType.MESH
F32 = jnp.float32
BF16 = jnp.bfloat16
NT = (((1,), (1,)), ((), ()))
NN = (((1,), (0,)), ((), ()))


def split(x):
    hi = x.astype(BF16)
    return hi, (x - hi.astype(F32)).astype(BF16)


def dot3(x_hi_lo, x_hi, w_hi, w_lo, dims):
    n = x_hi.shape[0]
    both = lax.dot_general(x_hi_lo, w_hi, dims, preferred_element_type=F32)
    low = lax.dot_general(x_hi, w_lo, dims, preferred_element_type=F32)
    return both[:n] + both[n:] + low


def kernel(nka, nga, cfg, m_ref, e_ref, c_ref, s_ref, al_ref, be_ref, out_ref,
           mhi, mlo, r, prev, xs, ws, tx, rx, acc, full, ypart, rtx, ltx, rrx, lrx,
           row_tx, ka_rx, ga_tx, ga_rx, *rest):
    nb, gw, cw, nch, nv = cfg
    stage_rx = rest[:nb]
    (core_ss, core_rs, st_ss, st_rs, ag_ss, ag_rs, fin_ss, fin_rs,
     r_ss, r_rs, l_ss, l_rs, ka_ss, ka_rs, ga_ss, ga_rs) = rest[nb:]
    ka = lax.axis_index("ka")
    ga = lax.axis_index("ga")
    core = ka % 2
    rows, gs = m_ref.shape
    gh = gs // 2

    def flip(mask):
        return ka + mask - 2 * mask * ((ka // mask) % 2)

    def bit_of(mask):
        return (ka // mask) % 2

    partners, bits = [], []
    for t in range(nb):
        a, b = 2 << t, 2 << (nb - 1 - t)
        partners.append(flip(a) + core * (flip(b) - flip(a)))
        bits.append(bit_of(a) + core * (bit_of(b) - bit_of(a)))

    barrier = pltpu.get_barrier_semaphore()
    for i in range(1, nka):
        pl.semaphore_signal(barrier, inc=1, device_id=((ka + i) % nka, ga), device_id_type=MESH)
    for i in range(1, nga):
        pl.semaphore_signal(barrier, inc=1, device_id=(ka, (ga + i) % nga), device_id_type=MESH)

    @pl.loop(0, rows // 128)
    def _(i):
        sl = pl.ds(pl.multiple_of(i * 128, 128), 128)
        hi, lo = split(m_ref[sl, :])
        mhi[sl, :] = hi
        mlo[sl, :] = lo
        r[:, sl] = s_ref[sl, :].T

    prev[...] = jnp.zeros_like(prev)
    pl.semaphore_wait(barrier, nka - 1 + nga - 1)

    def copy(src, dst, ss, rs, dev):
        return pltpu.make_async_remote_copy(
            src_ref=src, dst_ref=dst, send_sem=ss, recv_sem=rs, device_id=dev, device_id_type=MESH)

    def fold(x):
        parts = x[:, :128]
        for i in range(1, x.shape[1] // 128):
            parts = parts + x[:, i * 128:(i + 1) * 128]
        return jnp.sum(parts.T, axis=0, keepdims=True)

    def column(row):
        return jnp.broadcast_to(row, (128, nv)).T

    def wide(col, width):
        return jnp.concatenate([col] * (width // 128), axis=1)

    def small_copies(src, dst, ss, rs, n, me, dev, par):
        return [copy(src.at[par], dst.at[par, i], ss.at[i], rs.at[par, i], dev((me + i) % n))
                for i in range(1, n)]

    def ka_small(par):
        return small_copies(row_tx, ka_rx, ka_ss, ka_rs, nka, ka, lambda d: (d, ga), par)

    def ga_small(par):
        return small_copies(ga_tx, ga_rx, ga_ss, ga_rs, nga, ga, lambda d: (ka, d), par)

    def finish(copies, src, dst, n, par):
        for c in copies:
            c.wait()
        total = src[par]
        for i in range(1, n):
            total = total + dst[par, i]
        return total

    def project(half, write):
        @pl.loop(0, gh // gw)
        def _(i):
            dst = pl.ds(pl.multiple_of(i * gw, gw), gw)
            sl = pl.ds(pl.multiple_of(half * gh + i * gw, gw), gw)
            write(dst, dot3(xs[...], xs[:nv, :], mhi[:, sl], mlo[:, sl], NN))

    def body(k, carry):
        par = k % 2
        x = r[...]
        hi, lo = split(x)
        xs[:nv, :] = hi
        xs[nv:, :] = lo
        sq = x * x
        row_tx[par, 0:1, :] = fold(sq)
        row_tx[par, 1:2, :] = fold(e_ref[...] * sq)
        sums = ka_small(par)
        for c in sums:
            c.start()

        def to_tx(dst, y):
            tx[:, dst] = y

        def to_acc(dst, y):
            acc[:, dst] = y

        other = ka + 1 - 2 * core
        project(1 - core, to_tx)
        first = copy(tx, rx.at[par], core_ss.at[0], core_rs.at[par], (other, ga))
        first.start()
        project(core, to_acc)
        first.wait()
        acc[...] += rx[par]

        off, size = 0, nv
        spans = []
        for t in range(nb - 1):
            size //= 2
            keep = pl.multiple_of(off + bits[t] * size, 8)
            give = pl.multiple_of(off + (1 - bits[t]) * size, 8)
            c = copy(acc.at[pl.ds(give, size), :], stage_rx[t].at[par], st_ss.at[t], st_rs.at[par, t],
                     (partners[t], ga))
            c.start()
            c.wait()
            acc[pl.ds(keep, size), :] += stage_rx[t][par]
            off = keep
            spans.append((keep, size))
        t = nb - 1
        mine = pl.ds(off, size)
        c = copy(acc.at[mine, :], stage_rx[t].at[par], st_ss.at[t], st_rs.at[par, t], (partners[t], ga))
        c.start()
        c.wait()
        full[par, core, mine, :] = acc[mine, :] + stage_rx[t][par]
        for t in reversed(range(nb - 1)):
            keep, size = spans[t]
            part = full.at[par, core, pl.ds(keep, size), :]
            c = copy(part, part, ag_ss.at[t], ag_rs.at[par, t], (partners[t], ga))
            c.start()
            c.wait()
        part = full.at[par, core]
        c = copy(part, part, fin_ss.at[0], fin_rs.at[par], (other, ga))
        c.start()

        total = finish(sums, row_tx, ka_rx, nka, par)
        beta = jnp.sqrt(total[0:1] + EPSILON)
        energy = total[1:2] / (beta * beta)
        be_ref[pl.ds(jnp.maximum(k - 1, 0), 1), :] = beta
        beta_col = column(beta)
        c.wait()

        curve = jnp.zeros((nv, 128), F32)
        for h in range(2):
            for i in range(gh // 128):
                sl = slice(i * 128, (i + 1) * 128)
                gsl = slice(h * gh + i * 128, h * gh + (i + 1) * 128)
                p = full[par, h, :, sl] / beta_col
                w = c_ref[:, gsl] * p
                curve = curve + p * w
                hi, lo = split(w)
                ws[:nv, gsl] = hi
                ws[nv:, gsl] = lo
        ga_tx[par, 0:1, :] = fold(curve)
        curves = ga_small(par)
        for c in curves:
            c.start()

        def right(j):
            return copy(rtx.at[j], rrx.at[par, j], r_ss.at[j], r_rs.at[par, j], (ka, ga + 1))

        def left(j):
            return copy(ltx.at[j], lrx.at[par, j], l_ss.at[j], l_rs.at[par, j], (ka, ga - 1))

        @pl.loop(0, nch)
        def _(j):
            sl = pl.ds(pl.multiple_of(j * cw, cw), cw)
            y = dot3(ws[...], ws[:nv, :], mhi[sl, :], mlo[sl, :], NT)
            for h in range(2):
                i = 2 * j + h
                part = y[h * nv // 2:(h + 1) * nv // 2]
                ypart[i] = part

                @pl.when(ga == 0)
                def _():
                    rtx[i] = part
                    right(i).start()

                @pl.when(ga == nga - 1)
                def _():
                    ltx[i] = part
                    left(i).start()

        beta_wide = wide(beta_col, rows)
        r[...] = r[...] / beta_wide
        @pl.loop(0, 2 * nch + nga - 1)
        def _(t):
            jr = t - ga
            jl = t - (nga - 1 - ga)

            @pl.when((ga > 0) & (jr >= 0) & (jr < 2 * nch))
            def _():
                right(jr).wait_recv()

                @pl.when(ga < nga - 1)
                def _():
                    rtx[jr] = rrx[par, jr] + ypart[jr]
                    right(jr).start()

            @pl.when((ga < nga - 1) & (jl >= 0) & (jl < 2 * nch))
            def _():
                left(jl).wait_recv()

                @pl.when(ga > 0)
                def _():
                    ltx[jl] = lrx[par, jl] + ypart[jl]
                    left(jl).start()

        alpha = energy + finish(curves, ga_tx, ga_rx, nga, par)[0:1]
        al_ref[pl.ds(k, 1), :] = alpha
        alpha_col = wide(column(alpha), cw)
        beta_col = wide(beta_col, cw)
        for j in range(nch):
            sl = slice(j * cw, (j + 1) * cw)

            for i in (2 * j, 2 * j + 1):
                @pl.when(ga > 0)
                def _():
                    ypart[i] += rrx[par, i]

                @pl.when(ga < nga - 1)
                def _():
                    ypart[i] += lrx[par, i]

            v = r[:, sl]
            mixed = jnp.concatenate([ypart[2 * j], ypart[2 * j + 1]], axis=0)
            new = (e_ref[:, sl] - alpha_col) * v + mixed - beta_col * prev[:, sl]
            prev[:, sl] = v
            r[:, sl] = new
        for j in range(2 * nch):
            @pl.when(ga < nga - 1)
            def _():
                right(j).wait_send()

            @pl.when(ga > 0)
            def _():
                left(j).wait_send()
        return carry

    lax.fori_loop(0, ITERS, body, 0)
    par = ITERS % 2
    x = r[...]
    row_tx[par, 0:1, :] = fold(x * x)
    sums = ka_small(par)
    for c in sums:
        c.start()
    total = finish(sums, row_tx, ka_rx, nka, par)
    beta = jnp.sqrt(total[0:1] + EPSILON)
    be_ref[ITERS - 1:ITERS, :] = beta
    for j in range(rows // 128):
        sl = slice(j * 128, (j + 1) * 128)
        out_ref[sl, :] = r[:, sl].T / beta


def solution(mesh):
    nka, nga = mesh.shape["ka"], mesh.shape["ga"]
    nb = (nka // 2).bit_length() - 1

    def step(m, e, c, s):
        rows, gs = m.shape
        nv = s.shape[1]
        gh = gs // 2
        gw = min(512, gh)
        cw = 256
        nch = rows // cw
        stage = []
        for t in range(nb):
            size = nv >> (t + 1) if t < nb - 1 else nv >> (nb - 1)
            stage.append(pltpu.VMEM((2, size, gh), F32))
        vm = pltpu.VMEM
        dma = pltpu.SemaphoreType.DMA
        return pl.pallas_call(
            functools.partial(kernel, nka, nga, (nb, gw, cw, nch, nv)),
            out_shape=(jax.ShapeDtypeStruct((ITERS, nv), F32), jax.ShapeDtypeStruct((ITERS, nv), F32),
                       jax.ShapeDtypeStruct((rows, nv), F32)),
            in_specs=[pl.BlockSpec(memory_space=pltpu.VMEM)] * 4,
            out_specs=(pl.BlockSpec(memory_space=pltpu.VMEM),) * 3,
            scratch_shapes=[
                vm((rows, gs), BF16), vm((rows, gs), BF16), vm((nv, rows), F32), vm((nv, rows), F32),
                vm((2 * nv, rows), BF16), vm((2 * nv, gs), BF16),
                vm((nv, gh), F32), vm((2, nv, gh), F32), vm((nv, gh), F32), vm((2, 2, nv, gh), F32),
                vm((2 * nch, nv // 2, cw), F32), vm((2 * nch, nv // 2, cw), F32), vm((2 * nch, nv // 2, cw), F32),
                vm((2, 2 * nch, nv // 2, cw), F32), vm((2, 2 * nch, nv // 2, cw), F32),
                vm((2, 8, nv), F32), vm((2, nka, 8, nv), F32), vm((2, 8, nv), F32), vm((2, nga, 8, nv), F32),
            ] + stage + [
                dma((1,)), dma((2,)), dma((nb,)), dma((2, nb)), dma((nb,)), dma((2, nb)), dma((1,)), dma((2,)),
                dma((2 * nch,)), dma((2, 2 * nch)), dma((2 * nch,)), dma((2, 2 * nch)),
                dma((nka,)), dma((2, nka)), dma((nga,)), dma((2, nga)),
            ],
            compiler_params=pltpu.CompilerParams(
                collective_id=0, has_side_effects=True, vmem_limit_bytes=60 * 1024 * 1024),
        )(m, e[None, :], c[None, :], s)

    placed = (P("ka", "ga"), P("ka"), P("ga"), P("ka", None))
    return jax.shard_map(
        step, mesh=mesh, in_specs=placed, out_specs=(P(), P(), P("ka", None)), check_vma=False)
```
